32 devices in a mesh: section: 2 (over core), dp: 16 (over z, y, x).
Axes of the slice: x: 2, y: 2, z: 4, core: 2. Of those that a mesh axis runs over, the one named last changes fastest.
Arguments:
- ends: bfloat16 [2, 2, 96, 256, 384], P('section', None, 'dp'), may hold values from -6 to 6
- counts: int32 [2, 16], P(None, 'dp'), may hold values from 1 to 6, as said below
- qkv_weight: bfloat16 [2, 384, 1152], P('section', 'dp'), may hold values from -0.3125 to 0.3125
- out_weight: bfloat16 [2, 384, 384], P('section', 'dp'), may hold values from -1.25 to 1.25
- up_weight: bfloat16 [2, 384, 1536], P('section', 'dp'), may hold values from -0.3125 to 0.3125
- down_weight: bfloat16 [2, 1536, 384], P('section', 'dp'), may hold values from -0.15625 to 0.15625
- norm_gains: bfloat16 [2, 2, 384], P('section', None, 'dp'), may hold values from 0.5 to 1.5
- norm_shifts: bfloat16 [2, 2, 384], P('section', None, 'dp'), may hold values from -3 to 3
- up_bias: bfloat16 [2, 1536], P('section', 'dp'), may hold values from -3 to 3
Outputs:
- ends_out: float32 [2, 2, 96, 256, 384], P('section', None, 'dp')
- qkv_grad: float32 [2, 384, 1152], P('section', 'dp')
- out_grad: float32 [2, 384, 384], P('section', 'dp')
- up_grad: float32 [2, 384, 1536], P('section', 'dp')
- down_grad: float32 [2, 1536, 384], P('section', 'dp')
- gains_grad: float32 [2, 2, 384], P('section', None, 'dp')
- shifts_grad: float32 [2, 2, 384], P('section', None, 'dp')
- up_bias_grad: float32 [2, 1536], P('section', 'dp')
The draws below stay inside these ranges and needn't reach their ends.
Inputs may be any that keep to these rules, and one draw needn't show every extreme that they name: `counts`: in every micro-batch some dp index runs exactly 6 images.
All inputs are finite; a program needn't handle non-finite values.
Results may differ from the reference program's by a relative error of at most 0.0089.
Values may be sent and summed in bfloat16 or wider, within the bound.
A program may use at most 256 MiB of HBM per device.

```python
import math
from functools import partial
import jax
import jax.numpy as jnp
from jax import lax

D = 384
H = 6
HD = 64
FF = 1536
PAD = 256
SEQ = 197
MB = 2
CAP = 6
SLOTS = 96
N_DP = 16


def draw_counts(key, part):
    base = jax.random.randint(key, (MB, N_DP), 1, CAP + 1)
    chosen = jax.random.randint(jax.random.fold_in(key, 1), (MB, 1), 0, N_DP)
    filled = jnp.arange(N_DP)[None, :] == chosen
    return jnp.where(filled, CAP, base).astype(jnp.int32)


def steps_of(stream_key, shape, pieces, low, largest):
    level, own = 1.0, jax.random.fold_in(stream_key, 6)
    for position, shards_of in pieces:
        heights = jnp.exp(jax.random.uniform(jax.random.fold_in(own, position), (shards_of,), jnp.float32, low / len(pieces), largest / len(pieces)))
        level = level * jnp.repeat(heights, shape[position] // shards_of).reshape([-1 if axis == position else 1 for axis in range(len(shape))])
    return level


def scatter_about(stream_key, extent, deviation, bound, pieces=(), held_as=jnp.bfloat16):
    drawn = deviation * jax.random.normal(stream_key, extent, jnp.float32)
    if pieces:
        drawn = drawn * steps_of(stream_key, extent, pieces, -0.22, 0.18)
    return jnp.clip(drawn, -bound, bound).astype(held_as)


def setup_inputs(seed: int = 0) -> dict:
    arg_keys = jax.random.split(jax.random.key(seed), 10)
    ends = scatter_about(arg_keys[0], (2, MB, SLOTS, PAD, D), 1.0, 6.0, ((0, 2), (2, 16)))
    counts = draw_counts(jax.random.fold_in(arg_keys[9], 71), 0)
    qkv_weight = scatter_about(arg_keys[2], (2, D, 3 * D), D ** -0.5, 0.3125, ((0, 2), (1, 16)))
    out_weight = scatter_about(arg_keys[3], (2, D, D), (D // 14) ** -0.5, 1.25, ((0, 2), (1, 16)))
    up_weight = scatter_about(arg_keys[4], (2, D, FF), D ** -0.5, 0.3125, ((0, 2), (1, 16)))
    down_weight = scatter_about(arg_keys[5], (2, FF, D), FF ** -0.5, 0.15625, ((0, 2), (1, 16)))
    norm_gains = jnp.clip(1.0 + 0.1 * jax.random.normal(arg_keys[6], (2, 2, D), jnp.float32), 0.5, 1.5).astype(jnp.bfloat16)
    norm_shifts = scatter_about(arg_keys[7], (2, 2, D), 0.5, 3.0, ((0, 2), (2, 16)))
    up_bias = scatter_about(arg_keys[8], (2, FF), 0.5, 3.0, ((0, 2), (1, 16)))
    return {"ends": ends, "counts": counts, "qkv_weight": qkv_weight, "out_weight": out_weight, "up_weight": up_weight, "down_weight": down_weight, "norm_gains": norm_gains, "norm_shifts": norm_shifts, "up_bias": up_bias}


EPS = 1e-06

@jax.custom_vjp
def low(v):
    return lax.optimization_barrier(v.astype(jnp.bfloat16)).astype(jnp.float32)

@jax.custom_vjp
def low_back(v):
    return v

def low_keep(v):
    return (low(v), None)

def low_pass(kept, grad):
    return (grad,)

def back_keep(v):
    return (v, None)

def back_low(kept, grad):
    return (low(grad),)
low.defvjp(low_keep, low_pass)
low_back.defvjp(back_keep, back_low)

def normalize(values, gain, shift):
    centred = values - lax.optimization_barrier(jnp.mean(values, -1, keepdims=True))
    inverse = lax.rsqrt(lax.optimization_barrier(jnp.mean(centred * centred, -1, keepdims=True)) + EPS)
    return centred * inverse * gain + shift

def product(left, right):
    return jnp.dot(left, right, precision=lax.Precision.HIGHEST, preferred_element_type=jnp.float32)

def one_image(tokens_in, weights):
    w_qkv, w_out, w_up, w_down, gain_rows, shift_rows, up_shift = weights
    normed = low(normalize(tokens_in, gain_rows[0], shift_rows[0]))
    packed = low(low_back(product(normed, w_qkv))).reshape(PAD, 3, H, HD)
    scale = 1.0 / math.sqrt(HD)
    scores = low_back(scale * jnp.einsum('qhd,khd->hqk', packed[:, 0], packed[:, 1], precision=lax.Precision.HIGHEST))
    token_valid = jnp.arange(PAD) < SEQ
    scores = jnp.where(token_valid[None, None, :], scores, -1e+30)
    shifted = jnp.exp(scores - lax.optimization_barrier(jnp.max(scores, -1, keepdims=True)))
    soft = low(shifted / lax.optimization_barrier(jnp.sum(shifted, -1, keepdims=True)))
    attended = jnp.einsum('hqk,khd->qhd', soft, packed[:, 2], precision=lax.Precision.HIGHEST).reshape(PAD, H * HD)
    attended = low(low_back(attended))
    middle = tokens_in + low_back(product(attended, w_out))
    normed_two = low(normalize(middle, gain_rows[1], shift_rows[1]))
    pre_act = low_back(product(normed_two, w_up) + up_shift)
    hidden = low(jax.nn.gelu(pre_act, approximate=False))
    return middle + low_back(product(hidden, w_down))

def section_run(section_number, tokens, weight_set):
    weights = tuple((item[section_number] for item in weight_set))

    def per_image(image):
        return one_image(image, weights)
    return lax.map(jax.checkpoint(per_image), tokens)

def forward(inputs, w_qkv, w_out, w_up, w_down, gains, shifts, up_shift, live):
    weight_set = (w_qkv, w_out, w_up, w_down, gains, shifts, up_shift)
    first_out = section_run(0, inputs, weight_set)
    passed = low(low_back(first_out))
    second_out = section_run(1, passed, weight_set)
    return second_out * live

def reference(ends, counts, qkv_weight, out_weight, up_weight, down_weight, norm_gains, norm_shifts, up_bias):
    inputs = ends[0].astype(jnp.float32).reshape(MB * SLOTS, PAD, D)
    cotangent = ends[1].astype(jnp.float32).reshape(MB * SLOTS, PAD, D)
    slot_ids = jnp.arange(SLOTS)
    owner = slot_ids // CAP
    within = slot_ids % CAP
    live_slot = within[None, :] < counts[:, owner]
    token_valid = jnp.arange(PAD) < SEQ
    live = (live_slot[:, :, None] & token_valid[None, None, :]).astype(jnp.float32).reshape(MB * SLOTS, PAD, 1)
    weights = tuple((item.astype(jnp.float32) for item in (qkv_weight, out_weight, up_weight, down_weight, norm_gains, norm_shifts, up_bias)))
    result, pull = jax.vjp(partial(forward, live=live), inputs, *weights)
    grads = pull(cotangent)
    ends_out = jnp.stack([grads[0], result]).reshape(2, MB, SLOTS, PAD, D)
    return (ends_out, grads[1], grads[2], grads[3], grads[4], grads[5], grads[6], grads[7])
```

```python
import functools
import math

import jax, jax.numpy as jnp
from jax import lax
from jax.experimental import pallas as pl
from jax.experimental.pallas import tpu as pltpu
from jax.sharding import PartitionSpec as P

D = 384; H = 6; HD = 64; FF = 1536; PAD = 256; SEQ = 197
R = 208
EPS = 1e-06
SQRT_HALF = 0.7071067811865476
INV_ROOT_TWO_PI = 0.3989422804014327
F32 = jnp.float32; BF = jnp.bfloat16

def nn(a, b):
    return jnp.dot(a, b, preferred_element_type=F32)
def nt(a, b):
    return lax.dot_general(a, b, (((1,), (1,)), ((), ())), preferred_element_type=F32)
def tn(a, b):
    return lax.dot_general(a, b, (((0,), (0,)), ((), ())), preferred_element_type=F32)

def unit(v):
    c = v - jnp.mean(v, -1, keepdims=True)
    r = lax.rsqrt(jnp.mean(c * c, -1, keepdims=True) + EPS)
    return c * r, r

def low_half():
    return lax.broadcasted_iota(jnp.int32, (1, 128), 1) < HD

def fwd_attn(x, W, S, i):
    z, _ = unit(x)
    n1 = (z * W['g'][0:1] + W['c'][0:1]).astype(BF)
    S['n1'][i] = n1
    S['qkv'][i, 0:R] = nn(n1, W['qkv'][...]).astype(BF)
    half = low_half()
    real = lax.broadcasted_iota(jnp.int32, (1, PAD), 1) < SEQ
    for p in range(H // 2):
        a = p * 128
        q = S['qkv'][i, 0:R, a:a + 128]
        k = S['qkv'][i, :, D + a:D + a + 128]
        v = S['qkv'][i, :, 2 * D + a:2 * D + a + 128]
        qs = q * jnp.asarray(0.125, BF)
        zero = jnp.zeros_like(qs)
        outs, rls = [], []
        for h in range(2):
            qm = jnp.where(half if h == 0 else ~half, qs, zero)
            s = jnp.where(real, nt(qm, k), -1e30)
            e = jnp.exp(s - jnp.max(s, -1, keepdims=True))
            l = jnp.sum(e, -1, keepdims=True)
            eb = e.astype(BF)
            S['E'][i, (2 * p + h) * R:(2 * p + h + 1) * R] = eb
            outs.append(nn(eb, v)); rls.append(1.0 / l)
        rl = jnp.where(half, rls[0], rls[1])
        S['rl'][i, :, a:a + 128] = rl
        S['att'][i, :, a:a + 128] = (jnp.where(half, outs[0], outs[1]) * rl).astype(BF)
    S['mid'][i] = x + nn(S['att'][i], W['out'][...])

CH = 256
def fwd_mlp(W, S, i):
    mid = S['mid'][i]
    z, _ = unit(mid)
    n2 = (z * W['g'][1:2] + W['c'][1:2]).astype(BF)
    S['n2'][i] = n2
    for j in range(FF // CH):
        sl = slice(j * CH, (j + 1) * CH)
        u = nn(n2, W['up'][:, sl]) + W['ub'][0:1, sl]
        phi = 0.5 * (1.0 + lax.erf(u * SQRT_HALF))
        S['f'][i, :, sl] = (u * phi).astype(BF)
        S['sl'][i, :, sl] = (phi + u * (jnp.exp(-0.5 * u * u) * INV_ROOT_TWO_PI)).astype(BF)
    return mid + nn(S['f'][i], W['down'][...])

def norm_back(g_out, z, r, gain):
    t = g_out * gain
    gi = r * (t - jnp.mean(t, -1, keepdims=True) - z * jnp.mean(t * z, -1, keepdims=True))
    return gi, jnp.sum(g_out * z, 0, keepdims=True), jnp.sum(g_out, 0, keepdims=True)

def bwd_mlp(gm, W, S, i, G):
    G['down'][...] += tn(S['f'][i], gm)
    for j in range(FF // CH):
        sl = slice(j * CH, (j + 1) * CH)
        gu = (nt(gm, W['down'][sl, :]) * S['sl'][i, :, sl].astype(F32)).astype(BF)
        S['gu'][:, sl] = gu
        G['ub'][0:1, sl] += jnp.sum(gu.astype(F32), 0, keepdims=True)
    gu = S['gu'][...]
    G['up'][...] += tn(S['n2'][i], gu)
    gn = nt(gu, W['up'][...])
    z, r = unit(S['mid'][i])
    gi, dg, dc = norm_back(gn, z, r, W['g'][1:2])
    G['g'][1:2] += dg
    G['c'][1:2] += dc
    S['gmid'][i] = gm.astype(F32) + gi

def bwd_attn(x, W, S, i, G):
    gmid = S['gmid'][i]
    ga = gmid.astype(BF)
    att_all = S['att'][i]
    G['out'][...] += tn(att_all, ga)
    S['gatt'][...] = nt(ga, W['out'][...]).astype(BF)
    half = low_half()
    for p in range(H // 2):
        a = p * 128
        k = S['qkv'][i, :, D + a:D + a + 128]
        v = S['qkv'][i, :, 2 * D + a:2 * D + a + 128]
        qs = S['qkv'][i, 0:R, a:a + 128] * jnp.asarray(0.125, BF)
        gat = S['gatt'][:, a:a + 128].astype(F32) * S['rl'][i, :, a:a + 128]
        prod = gat * S['att'][i, :, a:a + 128].astype(F32)
        gatb = gat.astype(BF)
        gq = gk = gv = None
        for h in range(2):
            hm = half if h == 0 else ~half
            d = jnp.sum(jnp.where(hm, prod, 0.0), -1, keepdims=True)
            gm = jnp.where(hm, gatb, jnp.zeros_like(gatb))
            eb = S['E'][i, (2 * p + h) * R:(2 * p + h + 1) * R]
            gs = (eb.astype(F32) * (nt(gm, v) - d)).astype(BF)
            gvh = tn(eb, gm)
            gqh = nn(gs, jnp.where(hm, k, jnp.zeros_like(k)))
            gkh = tn(gs, jnp.where(hm, qs, jnp.zeros_like(qs)))
            if h == 0:
                gq, gk, gv = gqh, gkh, gvh
            else:
                gq, gk, gv = gq + gqh, gk + gkh, gv + gvh
        S['gqkv'][:, a:a + 128] = (gq * 0.125).astype(BF)
        S['gqkv'][:, D + a:D + a + 128] = gk[0:R].astype(BF)
        S['gqkv'][:, 2 * D + a:2 * D + a + 128] = gv[0:R].astype(BF)
    gqkv = S['gqkv'][...]
    G['qkv'][...] += tn(S['n1'][i], gqkv)
    gn = nt(gqkv, W['qkv'][...])
    z, r = unit(x)
    gi, dg, dc = norm_back(gn, z, r, W['g'][0:1])
    G['g'][0:1] += dg
    G['c'][0:1] += dc
    return gmid + gi
N = 6
STATE = dict(n1=((R, D), BF), qkv=((PAD, 3 * D), BF), E=((H * R, PAD), BF), rl=((R, D), F32), att=((R, D), BF),
             mid=((R, D), F32), n2=((R, D), BF), f=((R, FF), BF), sl=((R, FF), BF), gmid=((R, D), F32))
SHARED = dict(gu=((R, FF), BF), gatt=((R, D), BF), gqkv=((R, 3 * D), BF))
def scratch():
    out, names = [], []
    for L, n in ((0, N), (1, 1)):
        for k, (s, t) in STATE.items():
            out.append(pltpu.VMEM((n,) + s, t)); names.append((L, k))
    for k, (s, t) in SHARED.items():
        out.append(pltpu.VMEM(s, t)); names.append((2, k))
    out.append(pltpu.VMEM((N, R, D), BF)); names.append((2, 'x1'))
    out.append(pltpu.VMEM((N, R, D), BF)); names.append((2, 'gy'))
    return out, names

def kern(stages, x_ref, g_ref, wqkv, wout, wup, wdown, gg, cc, ub, out_ref, gin_ref, dqkv, dout, dup, ddown, dg, dc, dub, *sc):
    _, names = scratch()
    S = [{}, {}]
    for (L, k), ref in zip(names, sc):
        for l in ((0, 1) if L == 2 else (L,)):
            S[l][k] = ref
    W = [dict(qkv=wqkv.at[l], out=wout.at[l], up=wup.at[l], down=wdown.at[l], g=gg.at[l], c=cc.at[l], ub=ub.at[l]) for l in range(2)]
    G = [dict(qkv=dqkv.at[l], out=dout.at[l], up=dup.at[l], down=ddown.at[l], g=dg.at[l], c=dc.at[l], ub=dub.at[l]) for l in range(2)]
    for r in (dqkv, dout, dup, ddown, dg, dc, dub):
        r[...] = jnp.zeros_like(r)
    for l in range(2):
        for i in range(N if l == 0 else 1):
            S[l]['qkv'][i, R:PAD] = jnp.zeros((PAD - R, 3 * D), BF)
    if 'z' in stages:
        out_ref[...] = jnp.zeros_like(out_ref); gin_ref[...] = jnp.zeros_like(gin_ref)
    def loop(name, f):
        if name in stages:
            lax.fori_loop(0, N, lambda i, c: (f(i), c)[1], 0)
    def f0a(i): fwd_attn(x_ref[i].astype(F32), W[0], S[0], i)
    def f0b(i): S[0]['x1'][i] = fwd_mlp(W[0], S[0], i).astype(BF)
    def fb1a(i):
        x = S[0]['x1'][i].astype(F32)
        fwd_attn(x, W[1], S[1], 0)
    def fb1b(i):
        out_ref[i, 0:R] = fwd_mlp(W[1], S[1], 0)
    def fb1c(i):
        bwd_mlp(g_ref[i], W[1], S[1], 0, G[1])
    def fb1d(i):
        x = S[0]['x1'][i].astype(F32)
        S[0]['gy'][i] = bwd_attn(x, W[1], S[1], 0, G[1]).astype(BF)
    def b0a(i): bwd_mlp(S[0]['gy'][i], W[0], S[0], i, G[0])
    def b0b(i): gin_ref[i, 0:R] = bwd_attn(x_ref[i].astype(F32), W[0], S[0], i, G[0])
    loop('a', f0a); loop('b', f0b)
    if 'F' in stages:
        def fb(i):
            fb1a(i); fb1b(i); fb1c(i); fb1d(i)
        lax.fori_loop(0, N, lambda i, c: (fb(i), c)[1], 0)
    loop('c', b0a); loop('d', b0b)

def call(stages='zabFcd'):
    sc, _ = scratch()
    f = jax.ShapeDtypeStruct
    outs = (f((N, PAD, D), F32), f((N, PAD, D), F32), f((2, D, 3 * D), F32), f((2, D, D), F32), f((2, D, FF), F32), f((2, FF, D), F32),
            f((2, 2, D), F32), f((2, 2, D), F32), f((2, 1, FF), F32))
    return pl.pallas_call(functools.partial(kern, stages), out_shape=outs,
        in_specs=[pl.BlockSpec(memory_space=pltpu.VMEM)] * 9, out_specs=tuple([pl.BlockSpec(memory_space=pltpu.VMEM)] * 9),
        scratch_shapes=sc, compiler_params=pltpu.CompilerParams(vmem_limit_bytes=67043328), name='compute_' + stages)


def swap(v):
    return lax.ppermute(v, "section", [(0, 1), (1, 0)])


def body(ends, counts, qkv_weight, out_weight, up_weight, down_weight, norm_gains, norm_shifts, up_bias):
    first = lax.axis_index("section") == 0
    n = lax.axis_size("dp")
    rows = qkv_weight.shape[1]
    wide = jnp.concatenate([qkv_weight[0], out_weight[0], up_weight[0]], 1)
    small = jnp.concatenate([norm_gains.reshape(-1), norm_shifts.reshape(-1), up_bias.reshape(-1)])
    wide = lax.all_gather(wide, "dp", axis=0, tiled=True)
    down = lax.all_gather(down_weight[0], "dp", axis=0, tiled=True)
    small = lax.all_gather(small, "dp", axis=0)
    def both(v):
        o = swap(v)
        return jnp.where(first, jnp.stack([v, o]), jnp.stack([o, v]))
    wide, down, small = both(wide), both(down), both(small)
    gains = small[:, :, :2 * rows].reshape(2, n, 2, rows).transpose(0, 2, 1, 3).reshape(2, 2, D).astype(F32)
    shifts = small[:, :, 2 * rows:4 * rows].reshape(2, n, 2, rows).transpose(0, 2, 1, 3).reshape(2, 2, D).astype(F32)
    ub = small[:, :, 4 * rows:].reshape(2, 1, FF).astype(F32)
    theirs = swap(jnp.where(first, ends[0, 1], ends[0, 0]))
    x = jnp.where(first, ends[0, 0], theirs)
    g = jnp.where(first, theirs, ends[0, 1])
    mine = jnp.where(first, counts[0, 0], counts[1, 0])
    live = ((lax.iota(jnp.int32, N)[:, None] < mine) & (lax.iota(jnp.int32, PAD)[None, :] < SEQ))[:, :, None]
    g = jnp.where(live, g, 0)[:, :R]
    res = call()(x[:, :R], g, wide[:, :, :3 * D], wide[:, :, 3 * D:4 * D], wide[:, :, 4 * D:], down, gains, shifts, ub)
    out = jnp.where(live, res[0], 0.0)
    gin = res[1]
    other = swap(jnp.where(first, out, gin))
    ends_out = jnp.where(first, jnp.stack([gin, other]), jnp.stack([other, out]))[None]

    def pair(v):
        own = jnp.where(first, v[0], v[1])
        o = swap(jnp.where(first, v[1], v[0]).astype(BF))
        return (own + o.astype(F32)).astype(BF)

    def owner(v):
        v = v.reshape(n, v.shape[0] // n, v.shape[1])
        return lax.all_to_all(v, "dp", 0, 0, tiled=True).astype(F32).sum(0)
    gw = owner(pair(jnp.concatenate(res[2:5], 2)))
    gd = owner(pair(res[5]))
    gs = jnp.concatenate([v.reshape(2, 2, n, rows).transpose(0, 2, 1, 3).reshape(2, n, 2 * rows) for v in res[6:8]] + [res[8].reshape(2, n, 4 * rows)], 2)
    gs = owner(pair(gs))[0]
    return (ends_out, gw[None, :, :3 * D], gw[None, :, 3 * D:4 * D], gw[None, :, 4 * D:], gd[None],
            gs[:2 * rows].reshape(1, 2, rows), gs[2 * rows:4 * rows].reshape(1, 2, rows), gs[4 * rows:][None])


def solution(mesh):
    w = P("section", "dp", None)
    io = P("section", None, "dp", None, None)
    nrm = P("section", None, "dp")
    return jax.shard_map(body, mesh=mesh, in_specs=(io, P(None, "dp"), w, w, w, w, nrm, nrm, P("section", "dp")),
                         out_specs=(io, w, w, w, w, nrm, nrm, P("section", "dp")), check_vma=False)
```
